32 devices in a mesh: dp: 1 (over z), ri: 4 (over y), co: 4 (over x), ro: 2 (over core).
Axes of the slice: x: 4, y: 4, z: 1, core: 2. Of those that a mesh axis runs over, the one named last changes fastest.
The devices are a block of a 4x4x8 slice.
Arguments:
- act_in: bfloat16 [32768, 5120], P(('dp', 'ro', 'ri'), 'co')
- weight: bfloat16 [5120, 5120], P(('ro', 'ri'), 'co')
Outputs:
- output: bfloat16 [32768, 5120], P(('dp', 'ro', 'ri', 'co'))
All inputs are finite; a program needn't handle non-finite values.
Results may differ from the reference program's by a relative error of at most 0.001.
Values are sent between devices in bfloat16 or wider.
A program may use at most 768 MiB of HBM per device.

```python
import jax
import jax.numpy as jnp

ROWS_TOTAL = 32768
D_IN = 5120
D_OUT = 5120


def setup_inputs(seed: int = 0, part: int = 0) -> dict:
    key = jax.random.key(seed)
    key_a = jax.random.fold_in(jax.random.fold_in(key, 1), part)
    key_b = jax.random.fold_in(key, 2)
    act_in = jax.random.normal(key_a, (ROWS_TOTAL, D_IN), jnp.float32)
    weight = jax.random.normal(key_b, (D_IN, D_OUT), jnp.float32) * (D_IN ** -0.5)
    return {"act_in": act_in.astype(jnp.bfloat16), "weight": weight.astype(jnp.bfloat16)}


def reference(act_in, weight):
    product = jnp.dot(act_in, weight, preferred_element_type=jnp.float32)
    return product.astype(jnp.bfloat16)
```

```python
import functools

import jax
import jax.numpy as jnp
from jax import lax
from jax.experimental import pallas as pl
from jax.experimental.pallas import tpu as pltpu
from jax.sharding import PartitionSpec as P

MESH = pl.DeviceIdType.MESH
VMEM = 48 * 1024 * 1024
PARTS = 5
FIRST = 3
PIECES = ((0, FIRST), (FIRST, PARTS))

_NEAR = [
    [(0, 0)], [(0, -1)], [(1, -1)], [(2, 0)], [(2, -1)], [(0, 1), (2, 1)], [(0, 2), (2, 2)], [(-1, -1)],
    [(1, 0), (-1, 0)], [(1, 2), (-1, 2)], [(1, 1), (-1, 1)],
]
_FAR = [
    [(1, 0)], [(1, -1)], [(0, -1)], [(-1, 0)], [(-1, -1)], [(1, 1), (-1, 1)], [(1, 2), (-1, 2)], [(2, -1)],
    [(0, 0), (2, 0)], [(0, 2), (2, 2)], [(0, 1), (2, 1)],
]
_FINAL = (21, 23, 25, 27, 28, 29, 30, 31)

_EVENTS = [((-1, 0), 0), ((1, 0), 0), ((0, -1), 0), ((0, 1), 0), ((-1, 0), 1), ((1, 0), 1), ((0, -1), 1), ((0, 1), 1), ((-1, -1), 0), ((-1, 1), 0), ('T', 0), ((-1, -1), 1), ((-1, 1), 1), ('T', 1), ((-1, 2), 0), ((1, 1), 0), ('L', 0), ((2, 0), 0), ((-1, 2), 1), ((1, 1), 1), ((2, 0), 1), ('U', 0), ((1, -1), 0), ((2, 1), 0), ('E', 0), ('U', 1), ((1, -1), 1), ((2, 1), 1), ((2, -1), 0), ((2, -1), 1), ('Z', 0), ((0, 2), 0), ((2, 2), 0), ((0, 2), 1), ((1, 2), 0), ((2, 2), 1), ((1, 2), 1)]
_COUNTS = [17, 0, 0, 0, 0, 3, 6, 0, 2, 0, 0, 0, 0, 1, 0, 0, 1, 0, 1, 0, 1, 0, 2, 0, 0, 0, 2, 1, 0, 0, 0, 0]
_FRESH = (0, 5, 6, 16, 18, 20, 22, 26)


def order(table):
    return [(k, i, h) for row in table for h in range(2) for k, i in row]


def plan():
    events = _EVENTS
    out = []
    for count in _COUNTS:
        out.append(events[:count])
        events = events[count:]
    assert not events
    return out


def sends(event, near):
    what, h = event
    out = []
    if what in ("T", "U"):
        out = [("x", 1, "F", h)]
        if h and not near:
            out += [("x", 1, "T", 0), ("x", 1, "T", 1), ("x", 1, "H", 0)]
        if h and near:
            out += [("x", 1, (-1, 2), q) for q in range(2)]
    if isinstance(what, str):
        return out
    if what == (-1, 0):
        if not near:
            out = [("x", 1, what, h)]
        out += [("y", 1, what, h), ("y", -1, what, h)]
        if h and near:
            out += [("x", 1, "T", 0), ("x", 1, "T", 1), ("x", 1, what, 0), ("x", 1, what, 1), ("x", 1, "H", 0)]
    if what == (-1, 2) and not near:
        out = [("x", 1, what, h)]
    if what == (1, 0) and h:
        out = [("y", -1, what, q) for q in range(2)]
    if what == (2, 0):
        out = [("y", -1, what, h)]
        if h:
            out += [("y", 1, b, q) for b in ((2, 0), (0, -1)) for q in range(2)]
    if what == (-1, -1):
        out = [("y", 1, what, h)]
        if h:
            out += [("y", 1, b, q) for b in ((1, 0),) for q in range(2)]
    if what == (1, -1) and h == 0:
        out = [("y", 1, what, h)]
    if what == (0, 2) and h == 1:
        out = [("x", -1, what, h)]
    return out + [("c", 1, what, h)]


def first_sends():
    own = (0, 0)
    out = [(axis, s, own, h) for h in range(2) for s in (1, -1) for axis in "xy"]
    return out + [("x", -1, "L", 0)] + [("c", 1, own, h) for h in range(2)]


def kernel(nx, ny, a_ref, b_ref, o_ref, bg, av, transit, acc, bbuf,
           a_load, b_load, load_sem, recv_b, recv_a, send_sem):
    x, y, c = lax.axis_index("co"), lax.axis_index("ri"), lax.axis_index("ro")
    d = 1 - 2 * c
    xs = lambda i: lax.rem(x + i * d + 2 * nx, nx)
    ys = lambda j: lax.rem(y + j * d + 2 * ny, ny)
    target = lambda axis, s: {"co": xs(s)} if axis == "x" else {"ri": ys(s)} if axis == "y" else {"ro": 1 - c}
    rows, (kb, nb) = av.shape[1], b_ref.shape
    part, half = nb // PARTS, rows // 2

    barrier = pltpu.get_barrier_semaphore()
    for who in (target("x", 1), target("x", -1), target("y", 1), target("y", -1), target("c", 1)):
        pl.semaphore_signal(barrier, inc=1, device_id=who, device_id_type=MESH)
    pl.semaphore_wait(barrier, 5)

    def cols(h):
        first, last = PIECES[h]
        return pl.ds(first * part, (last - first) * part)

    def row_of(j):
        return c * ny + ys(j)

    def piece(r, n, h):
        return bg.at[r, n, :, cols(h)]

    def a_rows(s, first, count):
        return a_ref.at[pl.ds(pl.multiple_of(xs(s) * rows + first, half), count)]

    sent = []

    def push(send):
        axis, s, what, h = send
        if send not in sent:
            sent.append(send)
        index = sent.index(send)
        if isinstance(what, str):
            at = pl.ds(h * half, half)
            if what == "L":
                src, dst, recv = a_rows(-1, 0, rows), av.at[x], 0
            elif what == "H":
                src, dst, recv = a_rows(1, 0, rows), av.at[x], 1
            elif what == "T":
                src, dst, recv = a_rows(2, h * half, half), transit.at[h], 2 + h
            else:
                src, dst, recv = transit.at[h], av.at[xs(-1), at], 4 + h
            sems = send_sem.at[index], recv_a.at[recv]
        else:
            i, j = what
            r, n = row_of(j), xs(i)
            dst = piece(r, n, h)
            src = b_ref.at[:, cols(h)] if what == (0, 0) else dst
            sems = send_sem.at[index], recv_b.at[r, n, h]
        pltpu.make_async_remote_copy(
            src_ref=src, dst_ref=dst, send_sem=sems[0], recv_sem=sems[1],
            device_id=target(axis, s), device_id_type=MESH).start()

    def wait(ref, sem):
        pltpu.make_async_copy(ref, ref, sem).wait()

    def wait_b(r, n, h):
        wait(piece(r, n, h), recv_b.at[r, n, h])

    near = lax.rem(x, 2) == lax.div(y, 2)

    def only(want, action):
        pl.when(near if want else jnp.logical_not(near))(action)

    def wait_behind():
        wait(av.at[xs(-1)], recv_a.at[1])

    def wait_across():
        for q in range(2):
            wait(av.at[xs(2), pl.ds(q * half, half)], recv_a.at[4 + q])

    def handle(event):
        what, h = event
        if what in ("T", "U"):
            @functools.partial(only, what == "U")
            def _():
                wait(transit.at[h], recv_a.at[2 + h])
                for send in sends(event, what == "U"):
                    push(send)
            return
        if what == "L":
            wait(av.at[xs(1)], recv_a.at[0])
        elif what in ("E", "Z"):
            only(what == "E", wait_across)
            only(what == "Z", wait_behind)
        else:
            i, j = what
            wait_b(row_of(j), xs(i), h)
        both = [sends(event, want) for want in (False, True)]
        if both[0] == both[1]:
            for send in both[0]:
                push(send)
        else:
            for want in range(2):
                @functools.partial(only, want)
                def _():
                    for send in both[want]:
                        push(send)

    for send in first_sends():
        push(send)
    own_a = pltpu.make_async_copy(a_rows(0, 0, rows), av.at[x], a_load)
    own_a.start()
    own_b = [
        pltpu.make_async_copy(b_ref.at[:, cols(h)], bbuf.at[h, pl.ds(0, kb), pl.ds(0, cols(h).size)], b_load.at[h])
        for h in range(2)]
    for copy in own_b:
        copy.start()
    back = []
    for h in range(2):
        own_b[h].wait()
        back.append(pltpu.make_async_copy(
            bbuf.at[h, pl.ds(0, kb), pl.ds(0, cols(h).size)], piece(row_of(0), x, h), b_load.at[h]))
        back[h].start()

    def clear(n, _):
        acc[n] = jnp.zeros(acc.shape[1:], acc.dtype)
        return 0

    lax.fori_loop(0, acc.shape[0], clear, 0)
    for copy in back:
        copy.wait()
    own_a.wait()

    codes = [[(k + 1) * 8 + (i + 1) * 2 + h for k, i, h in order(t)] for t in (_NEAR, _FAR)]
    per = 6
    pack = lambda t, w: sum(v * 32 ** n for n, v in enumerate(t[w * per:(w + 1) * per]))
    words = [jnp.where(near, pack(codes[0], w), pack(codes[1], w)) for w in range(-(-len(codes[0]) // per))]

    def unit(s):
        w, m = lax.div(s, per), lax.rem(s, per)
        word = words[0]
        for n in range(1, len(words)):
            word = jnp.where(w == n, words[n], word)
        code = lax.rem(word, 32)
        for n in range(1, per):
            code = jnp.where(m == n, lax.rem(lax.div(word, 32 ** n), 32), code)
        k = xs(lax.div(code, 8) - 1)
        ro = lax.div(k, nx // 2)
        n = lax.rem(x + (lax.div(lax.rem(code, 8), 2) - 1) * (1 - 2 * ro) + 2 * nx, nx)
        return k, ro, n, lax.rem(code, 2)

    def fetch(s, what, start):
        k, ro, n, h = what
        p = lax.rem(s, 2)
        for hh in range(2):
            @pl.when(h == hh)
            def _():
                for q in range(2):
                    r = 2 * k + q
                    copy = pltpu.make_async_copy(
                        piece(r, n, hh), bbuf.at[p, pl.ds(q * kb, kb), pl.ds(0, cols(hh).size)], load_sem.at[p, q])
                    if start:
                        @pl.when(ro != c)
                        def _():
                            wait_b(r, n, hh)
                        copy.start()
                    else:
                        copy.wait()

    steps = plan()
    ahead = [t for t in range(1, len(steps)) if t not in _FRESH]

    def is_in(s, those):
        hit = s == -1
        for t in those:
            hit = jnp.logical_or(hit, s == t)
        return hit

    def step(s, this):
        for t, events in enumerate(steps):
            if events:
                @pl.when(s == t)
                def _():
                    for event in events:
                        handle(event)

        @pl.when(jnp.logical_not(is_in(s, ahead)))
        def _():
            fetch(s, this, True)

        after = unit(s + 1)

        @pl.when(is_in(s + 1, ahead))
        def _():
            fetch(s + 1, after, True)

        fetch(s, this, False)
        k, _, n, h = this
        p = lax.rem(s, 2)
        final = is_in(s, _FINAL)
        for hh, (first, last) in enumerate(PIECES):
            @pl.when(h == hh)
            def _():
                for g in range(first, last):
                    col = n * PARTS + g
                    acc[col] += jnp.dot(
                        av[k], bbuf[p, :, pl.ds((g - first) * part, part)], preferred_element_type=jnp.float32)

                @pl.when(final)
                def _():
                    for g in range(first, last):
                        col = n * PARTS + g
                        o_ref[:, pl.ds(pl.multiple_of(col * part, part), part)] = acc[col].astype(o_ref.dtype)
        return after

    lax.fori_loop(0, len(steps), step, unit(0))
    for n, (_, _, what, h) in enumerate(sent):
        ref = piece(0, 0, h) if not isinstance(what, str) else av.at[0] if what in "LH" else transit.at[0]
        wait(ref, send_sem.at[n])


def solution(mesh):
    nx, ny, nc = mesh.shape["co"], mesh.shape["ri"], mesh.shape["ro"]

    def local_block(a, b):
        rows, (kb, nb) = a.shape[0] // nx, b.shape
        kd, part = a.shape[1], nb // PARTS
        dma = pltpu.SemaphoreType.DMA
        all_sends = set(first_sends())
        for event in sum(plan(), []):
            for near in range(2):
                all_sends.update(sends(event, near))
        out, _ = pl.pallas_call(
            functools.partial(kernel, nx, ny),
            out_shape=(
                pltpu.VMEM((rows, nx * nb), jnp.bfloat16),
                jax.ShapeDtypeStruct((nc * ny, nx, kb, nb), jnp.bfloat16),
            ),
            in_specs=[pl.BlockSpec(memory_space=pl.ANY)] * 2,
            out_specs=(pl.BlockSpec(memory_space=pltpu.VMEM), pl.BlockSpec(memory_space=pl.ANY)),
            scratch_shapes=[
                pltpu.VMEM((nx, rows, kd), jnp.bfloat16),
                pltpu.VMEM((2, rows // 2, kd), jnp.bfloat16),
                pltpu.VMEM((nx * PARTS, rows, part), jnp.float32),
                pltpu.VMEM((2, 2 * kb, FIRST * part), jnp.bfloat16),
                dma, dma((2,)), dma((2, 2)),
                dma((nc * ny, nx, 2)), dma((6,)), dma((len(all_sends),)),
            ],
            compiler_params=pltpu.CompilerParams(
                collective_id=0, has_side_effects=True, vmem_limit_bytes=VMEM),
        )(a, b)
        return out

    return jax.shard_map(
        local_block,
        mesh=mesh,
        in_specs=(P(("dp", "ro", "ri"), "co"), P(("ro", "ri"), "co")),
        out_specs=P(("dp", "ro", "ri", "co"), None),
        check_vma=False,
    )
```

```python
import functools

import jax
import jax.numpy as jnp
from jax import lax
from jax.experimental import pallas as pl
from jax.experimental.pallas import tpu as pltpu
from jax.sharding import PartitionSpec as P

MESH = pl.DeviceIdType.MESH
VMEM = 48 * 1024 * 1024
PARTS = 5
FIRST = 3
PIECES = ((0, FIRST), (FIRST, PARTS))

_KINDS = (-1, 0, 1, 2, "side", "far")


def _unit(code):
    return _KINDS[code // 8], code // 2 % 4 - 1, code % 2


def _event(code):
    if isinstance(code, str):
        return code[0], len(code) - 1
    return (code // 8 - 1, code // 2 % 4 - 1), code % 2


_NEAR = [_unit(code) for code in (
    8, 10, 9, 17, 16, 11, 24, 27, 13, 25, 29, 26, 12, 14, 30, 28,
    15, 31, 1, 34, 0, 20, 38, 4, 35, 39, 21, 46, 5, 42, 43, 47,
)]
_FAR = [_unit(code) for code in (
    19, 9, 8, 17, 16, 18, 0, 1, 4, 2, 5, 21, 3, 22, 20, 6,
    23, 7, 25, 38, 24, 12, 34, 28, 39, 13, 35, 46, 29, 42, 43, 47,
)]

_EVENTS = [_event(code) for code in (
    2, 12, 9, 18, 13, 19, "T", 3, 0, 1, "TT", 6, 26, 8, "L", 5,
    4, 7, 27, 16, "U", 28, 20, 21, "E", 17, "UU", 24, 29, 25, "Z", 22,
    23, 30, 14, 15, 31,
)]
_COUNTS = [17, 2, 0, 0, 1, 1, 4, 0, 1, 0, 1, 0, 2, 0, 0, 0, 1, 1, 1, 0, 0, 0, 0, 1, 1, 0, 2, 0, 1, 0, 0, 0]
_FRESH = (0, 1, 6, 8, 16)


def order(table):
    return table


def is_last(unit, near):
    k, i, _ = unit
    return k == "far" or (i == 1 and k in ((1, -1) if near else (0, 2)))


def plan():
    events = _EVENTS
    out = []
    for count in _COUNTS:
        out.append(events[:count])
        events = events[count:]
    assert not events
    return out


def sends(event, near):
    what, h = event
    out = []
    if what in ("T", "U"):
        out = [("x", 1, "F", h)]
        if h and not near:
            out += [("x", 1, "T", 0), ("x", 1, "T", 1), ("x", 1, "H", 0)]
        if h and near:
            out += [("x", 1, (-1, 2), q) for q in range(2)]
    if isinstance(what, str):
        return out
    if what == (-1, 0):
        if not near:
            out = [("x", 1, what, h)]
        out += [("y", 1, what, h), ("y", -1, what, h)]
        if h and near:
            out += [("x", 1, "T", 0), ("x", 1, "T", 1), ("x", 1, what, 0), ("x", 1, what, 1), ("x", 1, "H", 0)]
    if what == (-1, 2) and not near:
        out = [("x", 1, what, h)]
    if what == (1, 0) and h:
        out = [("y", -1, what, q) for q in range(2)]
    if what == (2, 0):
        out = [("y", -1, what, h)]
        if h:
            out += [("y", 1, what, q) for q in range(2)]
    if what == (-1, -1):
        out = [("y", 1, what, h)]
        if h:
            out += [("y", 1, (1, 0), q) for q in range(2)]
    if what == (1, -1):
        out = [("y", 1, what, h)]
        if h:
            out += [("y", 1, (0, -1), 0)]
    if what == (2, -1) and h:
        out = out + [("x", -1, (-1, 2), 1)]
    return out + [("c", 1, what, h)]


def first_sends():
    own = (0, 0)
    out = [(axis, s, own, h) for h in range(2) for s in (1, -1) for axis in "xy"]
    return out + [("x", -1, "L", 0)] + [("c", 1, own, h) for h in range(2)]


def kernel(nx, ny, a_ref, b_ref, o_ref, bg, av, transit, acc, bbuf,
           a_load, b_load, load_sem, recv_b, recv_a, send_sem):
    x, y, c = lax.axis_index("co"), lax.axis_index("ri"), lax.axis_index("ro")
    d = 1 - 2 * c
    xs = lambda i: lax.rem(x + i * d + 2 * nx, nx)
    ys = lambda j: lax.rem(y + j * d + 2 * ny, ny)
    target = lambda axis, s: {"co": xs(s)} if axis == "x" else {"ri": ys(s)} if axis == "y" else {"ro": 1 - c}
    rows, (kb, nb) = av.shape[1], b_ref.shape
    part, half = nb // PARTS, rows // 2

    barrier = pltpu.get_barrier_semaphore()
    for who in (target("x", 1), target("x", -1), target("y", 1), target("y", -1), target("c", 1)):
        pl.semaphore_signal(barrier, inc=1, device_id=who, device_id_type=MESH)
    pl.semaphore_wait(barrier, 5)

    def cols(h):
        first, last = PIECES[h]
        return pl.ds(first * part, (last - first) * part)

    def row_of(j):
        return c * ny + ys(j)

    def piece(r, n, h):
        return bg.at[r, n, :, cols(h)]

    def a_rows(s, first, count):
        return a_ref.at[pl.ds(pl.multiple_of(xs(s) * rows + first, half), count)]

    sent = []

    def push(send):
        axis, s, what, h = send
        if send not in sent:
            sent.append(send)
        index = sent.index(send)
        if isinstance(what, str):
            at = pl.ds(h * half, half)
            if what == "L":
                src, dst, recv = a_rows(-1, 0, rows), av.at[x], 0
            elif what == "H":
                src, dst, recv = a_rows(1, 0, rows), av.at[x], 1
            elif what == "T":
                src, dst, recv = a_rows(2, h * half, half), transit.at[h], 2 + h
            else:
                src, dst, recv = transit.at[h], av.at[xs(-1), at], 4 + h
            sems = send_sem.at[index], recv_a.at[recv]
        else:
            i, j = what
            r, n = row_of(j), xs(i)
            dst = piece(r, n, h)
            src = b_ref.at[:, cols(h)] if what == (0, 0) else dst
            sems = send_sem.at[index], recv_b.at[r, n, h]
        pltpu.make_async_remote_copy(
            src_ref=src, dst_ref=dst, send_sem=sems[0], recv_sem=sems[1],
            device_id=target(axis, s), device_id_type=MESH).start()

    def wait(ref, sem):
        pltpu.make_async_copy(ref, ref, sem).wait()

    def wait_b(r, n, h):
        wait(piece(r, n, h), recv_b.at[r, n, h])

    near = lax.rem(x, 2) == lax.div(y, 2)

    def only(want, action):
        pl.when(near if want else jnp.logical_not(near))(action)

    def wait_behind():
        wait(av.at[xs(-1)], recv_a.at[1])

    def wait_across():
        for q in range(2):
            wait(av.at[xs(2), pl.ds(q * half, half)], recv_a.at[4 + q])

    def handle(event):
        what, h = event
        if what in ("T", "U"):
            @functools.partial(only, what == "U")
            def _():
                wait(transit.at[h], recv_a.at[2 + h])
                for send in sends(event, what == "U"):
                    push(send)
            return
        if what == "L":
            wait(av.at[xs(1)], recv_a.at[0])
        elif what in ("E", "Z"):
            only(what == "E", wait_across)
            only(what == "Z", wait_behind)
        else:
            i, j = what
            wait_b(row_of(j), xs(i), h)
        both = [sends(event, want) for want in (False, True)]
        if both[0] == both[1]:
            for send in both[0]:
                push(send)
        else:
            for want in range(2):
                @functools.partial(only, want)
                def _():
                    for send in both[want]:
                        push(send)

    for send in first_sends():
        push(send)
    own_a = pltpu.make_async_copy(a_rows(0, 0, rows), av.at[x], a_load)
    own_a.start()
    own_b = [
        pltpu.make_async_copy(b_ref.at[:, cols(h)], bbuf.at[h, pl.ds(0, kb), pl.ds(0, cols(h).size)], b_load.at[h])
        for h in range(2)]
    for copy in own_b:
        copy.start()
    back = []
    for h in range(2):
        own_b[h].wait()
        back.append(pltpu.make_async_copy(
            bbuf.at[h, pl.ds(0, kb), pl.ds(0, cols(h).size)], piece(row_of(0), x, h), b_load.at[h]))
        back[h].start()

    def clear(n, _):
        acc[n] = jnp.zeros(acc.shape[1:], acc.dtype)
        return 0

    lax.fori_loop(0, acc.shape[0], clear, 0)
    for copy in back:
        copy.wait()
    own_a.wait()

    def unit(t):
        both = []
        for table, is_near in ((_FAR, False), (_NEAR, True)):
            k, i, h = order(table)[t]
            if isinstance(k, str):
                shift = ny // 2
                row = lax.rem(y + shift, ny)
                if k == "side":
                    row = lax.rem(y + 1 - 2 * lax.rem(y, 2) + shift, ny)
                fields = (row, row + ny, lax.rem(x + i, nx))
            else:
                k = xs(k)
                ro = lax.div(k, nx // 2)
                fields = (2 * k, 2 * k + 1, lax.rem(x + i * (1 - 2 * ro) + 2 * nx, nx))
            both.append(fields + (h, int(is_last(order(table)[t], is_near))))
        return [jnp.where(near, v, u) for u, v in zip(*both)]

    base, per = 1024, 3
    words = []
    for t in range(len(_COUNTS)):
        r1, r2, n, h, final = unit(t)
        code = (r1 + 8 * r2 + 64 * n + 256 * h + 512 * final) * base ** (t % per)
        if t % per:
            words[-1] += code
        else:
            words.append(code)

    def decode(s):
        w, m = lax.div(s, per), lax.rem(s, per)
        word = words[0]
        for n in range(1, len(words)):
            word = jnp.where(w == n, words[n], word)
        code = word
        for n in range(1, per):
            code = jnp.where(m == n, lax.div(word, base ** n), code)
        code = lax.rem(code, base)
        out = []
        for size in (8, 8, 4, 2, 2):
            out.append(lax.rem(code, size))
            code = lax.div(code, size)
        return tuple(out)

    def fetch(s, this, start):
        n, h = this[2], this[3]
        p = lax.rem(s, 2)
        for hh in range(2):
            @pl.when(h == hh)
            def _():
                for q in range(2):
                    r = this[q]
                    copy = pltpu.make_async_copy(
                        piece(r, n, hh), bbuf.at[p, pl.ds(q * kb, kb), pl.ds(0, cols(hh).size)], load_sem.at[p, q])
                    if start:
                        @pl.when(lax.div(r, ny) != c)
                        def _():
                            wait_b(r, n, hh)
                        copy.start()
                    else:
                        copy.wait()

    steps = plan()
    ahead = [t for t in range(1, len(steps)) if t not in _FRESH]

    def is_in(s, those):
        hit = s == those[0]
        for t in those[1:]:
            hit = jnp.logical_or(hit, s == t)
        return hit

    def rows_of_a(r):
        return av[lax.div(r, 2), :, pl.ds(pl.multiple_of(lax.rem(r, 2) * kb, 128), kb)]

    def step(s, this):
        for t, events in enumerate(steps):
            if events:
                @pl.when(s == t)
                def _():
                    for event in events:
                        handle(event)

        @pl.when(is_in(s, _FRESH))
        def _():
            fetch(s, this, True)

        after = decode(s + 1)

        @pl.when(jnp.logical_not(is_in(s, [t - 1 for t in _FRESH if t] + [len(steps) - 1])))
        def _():
            fetch(s + 1, after, True)

        fetch(s, this, False)
        r1, r2, n, h, final = this
        p = lax.rem(s, 2)
        for hh, (first, last) in enumerate(PIECES):
            @pl.when(h == hh)
            def _():
                for g in range(first, last):
                    col = n * PARTS + g
                    lhs = jnp.concatenate([rows_of_a(r1), rows_of_a(r2)], axis=1)
                    acc[col] += jnp.dot(
                        lhs, bbuf[p, :, pl.ds((g - first) * part, part)], preferred_element_type=jnp.float32)

                @pl.when(final == 1)
                def _():
                    for g in range(first, last):
                        col = n * PARTS + g
                        o_ref[:, pl.ds(pl.multiple_of(col * part, part), part)] = acc[col].astype(o_ref.dtype)
        return after

    lax.fori_loop(0, len(steps), step, decode(0))
    for n, (_, _, what, h) in enumerate(sent):
        ref = piece(0, 0, h) if not isinstance(what, str) else av.at[0] if what in "LH" else transit.at[0]
        wait(ref, send_sem.at[n])


def solution(mesh):
    nx, ny, nc = mesh.shape["co"], mesh.shape["ri"], mesh.shape["ro"]

    def local_block(a, b):
        rows, (kb, nb) = a.shape[0] // nx, b.shape
        kd, part = a.shape[1], nb // PARTS
        dma = pltpu.SemaphoreType.DMA
        all_sends = set(first_sends())
        for event in sum(plan(), []):
            for near in range(2):
                all_sends.update(sends(event, near))
        out, _ = pl.pallas_call(
            functools.partial(kernel, nx, ny),
            out_shape=(
                pltpu.VMEM((rows, nx * nb), jnp.bfloat16),
                jax.ShapeDtypeStruct((nc * ny, nx, kb, nb), jnp.bfloat16),
            ),
            in_specs=[pl.BlockSpec(memory_space=pl.ANY)] * 2,
            out_specs=(pl.BlockSpec(memory_space=pltpu.VMEM), pl.BlockSpec(memory_space=pl.ANY)),
            scratch_shapes=[
                pltpu.VMEM((nx, rows, kd), jnp.bfloat16),
                pltpu.VMEM((2, rows // 2, kd), jnp.bfloat16),
                pltpu.VMEM((nx * PARTS, rows, part), jnp.float32),
                pltpu.VMEM((2, 2 * kb, FIRST * part), jnp.bfloat16),
                dma, dma((2,)), dma((2, 2)),
                dma((nc * ny, nx, 2)), dma((6,)), dma((len(all_sends),)),
            ],
            compiler_params=pltpu.CompilerParams(
                collective_id=0, has_side_effects=True, vmem_limit_bytes=VMEM),
        )(a, b)
        return out

    return jax.shard_map(
        local_block,
        mesh=mesh,
        in_specs=(P(("dp", "ro", "ri"), "co"), P(("ro", "ri"), "co")),
        out_specs=P(("dp", "ro", "ri", "co"), None),
        check_vma=False,
    )
```

```python
import functools

import jax
import jax.numpy as jnp
from jax import lax
from jax.experimental import pallas as pl
from jax.experimental.pallas import tpu as pltpu
from jax.sharding import PartitionSpec as P

MESH = pl.DeviceIdType.MESH
VMEM = 48 * 1024 * 1024
PARTS = 5
FIRST = 3
PIECES = ((0, FIRST), (FIRST, PARTS))

_KINDS = (-1, 0, 1, 2, "side", "far")


def _unit(code):
    return _KINDS[code // 8], code // 2 % 4 - 1, code % 2


def _event(code):
    if isinstance(code, str):
        return code[0], len(code) - 1
    return (code // 8 - 1, code // 2 % 4 - 1), code % 2


_NEAR = [_unit(code) for code in (
    8, 16, 17, 9, 10, 25, 11, 12, 29, 27, 26, 24, 28, 30, 14, 13,
    31, 15, 39, 38, 0, 34, 4, 35, 20, 1, 5, 46, 21, 47, 42, 43,
)]
_FAR = [_unit(code) for code in (
    9, 16, 19, 8, 17, 0, 18, 3, 1, 21, 2, 4, 20, 5, 6, 22,
    23, 7, 25, 35, 34, 24, 12, 28, 38, 39, 13, 46, 29, 47, 42, 43,
)]

_EVENTS = [_event(code) for code in (
    2, 3, 18, 19, 5, "T", 4, 0, 1, "TT", 13, 6, 8, 9, 12, "L",
    7, 26, 21, 27, 20, "E", 16, "U", 17, "UU", 28, 24, 29, 25, "Z", 22,
    23, 30, 31, 14, 15,
)]
_COUNTS = [18, 1, 1, 0, 1, 2, 1, 1, 1, 1, 0, 0, 1, 0, 2, 0, 0, 1, 0, 1, 0, 0, 0, 0, 2, 0, 0, 2, 1, 0, 0, 0]
_FRESH = (0, 5)


def order(table):
    return table


def is_last(unit, near):
    k, i, _ = unit
    return k == "far" or (i == 1 and k in ((1, -1) if near else (0, 2)))


def plan():
    events = _EVENTS
    out = []
    for count in _COUNTS:
        out.append(events[:count])
        events = events[count:]
    assert not events
    return out


def sends(event, near):
    what, h = event
    out = []
    if what in ("T", "U"):
        out = [("x", 1, "F", h)]
        if h and not near:
            out += [("x", 1, "T", 0), ("x", 1, "T", 1), ("x", 1, "H", 0)]
        if h and near:
            out += [("x", 1, (-1, 2), q) for q in range(2)]
    if isinstance(what, str):
        return out
    if what == (-1, 0):
        if not near:
            out = [("x", 1, what, h)]
        out += [("y", 1, what, h), ("y", -1, what, h)]
        if h and near:
            out += [("x", 1, "T", 0), ("x", 1, "T", 1), ("x", 1, what, 0), ("x", 1, what, 1), ("x", 1, "H", 0)]
    if what == (-1, 2) and not near:
        out = [("x", 1, what, h)]
    if what == (1, 0) and h:
        out = [("y", -1, what, q) for q in range(2)]
    if what == (2, 0):
        out = [("y", -1, what, h)]
        if h:
            out += [("y", 1, what, q) for q in range(2)]
    if what == (-1, -1):
        out = [("y", 1, what, h)]
        if h:
            out += [("y", 1, (1, 0), q) for q in range(2)]
    if what == (1, -1):
        out = [("y", 1, what, h)]
        if h:
            out += [("y", 1, (0, -1), 0), ("y", 1, (0, -1), "q")]
    if what == (1, 2) and h:
        out = out + [("x", -1, (-1, 2), "t")]
    return out + [("c", 1, what, h)]


def first_sends():
    own = (0, 0)
    out = [(axis, s, own, h) for h in range(2) for s in (1, -1) for axis in "xy"]
    return out + [("x", -1, "L", 0)] + [("c", 1, own, h) for h in range(2)]


def kernel(nx, ny, a_ref, b_ref, o_ref, bg, av, transit, acc, bbuf,
           a_load, b_load, load_sem, recv_b, recv_q, recv_a, send_sem):
    x, y, c = lax.axis_index("co"), lax.axis_index("ri"), lax.axis_index("ro")
    d = 1 - 2 * c
    xs = lambda i: lax.rem(x + i * d + 2 * nx, nx)
    ys = lambda j: lax.rem(y + j * d + 2 * ny, ny)
    target = lambda axis, s: {"co": xs(s)} if axis == "x" else {"ri": ys(s)} if axis == "y" else {"ro": 1 - c}
    rows, (kb, nb) = av.shape[1], b_ref.shape
    part, half = nb // PARTS, rows // 2

    barrier = pltpu.get_barrier_semaphore()
    for who in (target("x", 1), target("x", -1), target("y", 1), target("y", -1), target("c", 1)):
        pl.semaphore_signal(barrier, inc=1, device_id=who, device_id_type=MESH)
    pl.semaphore_wait(barrier, 5)

    def cols(h):
        first, last = PIECES[h]
        return pl.ds(first * part, (last - first) * part)

    def row_of(j):
        return c * ny + ys(j)

    def piece(r, n, h):
        return bg.at[r, n, :, cols(h)]

    def a_rows(s, first, count):
        return a_ref.at[pl.ds(pl.multiple_of(xs(s) * rows + first, half), count)]

    def rows_piece(r, n, h):
        if h == "q":
            return bg.at[r, n, pl.ds(0, kb // 4), cols(1)]
        if h == "t":
            return bg.at[r, n, pl.ds(kb // 4, kb - kb // 4), cols(1)]
        return piece(r, n, h)

    sent = []

    def push(send):
        axis, s, what, h = send
        if send not in sent:
            sent.append(send)
        index = sent.index(send)
        if isinstance(what, str):
            at = pl.ds(h * half, half)
            if what == "L":
                src, dst, recv = a_rows(-1, 0, rows), av.at[x], 0
            elif what == "H":
                src, dst, recv = a_rows(1, 0, rows), av.at[x], 1
            elif what == "T":
                src, dst, recv = a_rows(2, h * half, half), transit.at[h], 2 + h
            else:
                src, dst, recv = transit.at[h], av.at[xs(-1), at], 4 + h
            sems = send_sem.at[index], recv_a.at[recv]
        else:
            i, j = what
            r, n = row_of(j), xs(i)
            dst = rows_piece(r, n, h)
            src = b_ref.at[:, cols(h)] if what == (0, 0) else dst
            sems = send_sem.at[index], recv_q if h == "q" else recv_b.at[r, n, 1 if h == "t" else h]
        pltpu.make_async_remote_copy(
            src_ref=src, dst_ref=dst, send_sem=sems[0], recv_sem=sems[1],
            device_id=target(axis, s), device_id_type=MESH).start()

    def wait(ref, sem):
        pltpu.make_async_copy(ref, ref, sem).wait()

    def wait_b(r, n, h):
        wait(piece(r, n, h), recv_b.at[r, n, h])

    near = lax.rem(x, 2) == lax.div(y, 2)

    def only(want, action):
        pl.when(near if want else jnp.logical_not(near))(action)

    def wait_behind():
        wait(av.at[xs(-1)], recv_a.at[1])

    def wait_across():
        for q in range(2):
            wait(av.at[xs(2), pl.ds(q * half, half)], recv_a.at[4 + q])

    def handle(event):
        what, h = event
        if what in ("T", "U"):
            @functools.partial(only, what == "U")
            def _():
                wait(transit.at[h], recv_a.at[2 + h])
                for send in sends(event, what == "U"):
                    push(send)
            return
        if what == "L":
            wait(av.at[xs(1)], recv_a.at[0])
        elif what in ("E", "Z"):
            only(what == "E", wait_across)
            only(what == "Z", wait_behind)
        else:
            i, j = what
            if what == (0, 2) and h:
                r, n = row_of(j), xs(i)
                wait(rows_piece(r, n, "q"), recv_q)
                wait(rows_piece(r, n, "t"), recv_b.at[r, n, h])
            else:
                wait_b(row_of(j), xs(i), h)
        both = [sends(event, want) for want in (False, True)]
        if both[0] == both[1]:
            for send in both[0]:
                push(send)
        else:
            for want in range(2):
                @functools.partial(only, want)
                def _():
                    for send in both[want]:
                        push(send)

    for send in first_sends():
        push(send)
    own_a = pltpu.make_async_copy(a_rows(0, 0, rows), av.at[x], a_load)
    own_a.start()
    own_b = [
        pltpu.make_async_copy(b_ref.at[:, cols(h)], bbuf.at[h, pl.ds(0, kb), pl.ds(0, cols(h).size)], b_load.at[h])
        for h in range(2)]
    for copy in own_b:
        copy.start()
    back = []
    for h in range(2):
        own_b[h].wait()
        back.append(pltpu.make_async_copy(
            bbuf.at[h, pl.ds(0, kb), pl.ds(0, cols(h).size)], piece(row_of(0), x, h), b_load.at[h]))
        back[h].start()

    def clear(n, _):
        acc[n] = jnp.zeros(acc.shape[1:], acc.dtype)
        return 0

    lax.fori_loop(0, acc.shape[0], clear, 0)
    for copy in back:
        copy.wait()
    own_a.wait()

    def unit(t):
        both = []
        for table, is_near in ((_FAR, False), (_NEAR, True)):
            k, i, h = order(table)[t]
            if isinstance(k, str):
                shift = ny // 2
                row = lax.rem(y + shift, ny)
                if k == "side":
                    row = lax.rem(y + 1 - 2 * lax.rem(y, 2) + shift, ny)
                fields = (row, row + ny, lax.rem(x + i, nx))
            else:
                k = xs(k)
                ro = lax.div(k, nx // 2)
                fields = (2 * k, 2 * k + 1, lax.rem(x + i * (1 - 2 * ro) + 2 * nx, nx))
            both.append(fields + (h, int(is_last(order(table)[t], is_near))))
        return [jnp.where(near, v, u) for u, v in zip(*both)]

    base, per = 1024, 3
    words = []
    for t in range(len(_COUNTS)):
        r1, r2, n, h, final = unit(t)
        code = (r1 + 8 * r2 + 64 * n + 256 * h + 512 * final) * base ** (t % per)
        if t % per:
            words[-1] += code
        else:
            words.append(code)

    def decode(s):
        w, m = lax.div(s, per), lax.rem(s, per)
        word = words[0]
        for n in range(1, len(words)):
            word = jnp.where(w == n, words[n], word)
        code = word
        for n in range(1, per):
            code = jnp.where(m == n, lax.div(word, base ** n), code)
        code = lax.rem(code, base)
        out = []
        for size in (8, 8, 4, 2, 2):
            out.append(lax.rem(code, size))
            code = lax.div(code, size)
        return tuple(out)

    def fetch(s, this, start):
        n, h = this[2], this[3]
        p = lax.rem(s, 2)
        for hh in range(2):
            @pl.when(h == hh)
            def _():
                for q in range(2):
                    r = this[q]
                    copy = pltpu.make_async_copy(
                        piece(r, n, hh), bbuf.at[p, pl.ds(q * kb, kb), pl.ds(0, cols(hh).size)], load_sem.at[p, q])
                    if start:
                        @pl.when(lax.div(r, ny) != c)
                        def _():
                            wait_b(r, n, hh)
                        copy.start()
                    else:
                        copy.wait()

    steps = plan()
    ahead = [t for t in range(1, len(steps)) if t not in _FRESH]

    def is_in(s, those):
        hit = s == those[0]
        for t in those[1:]:
            hit = jnp.logical_or(hit, s == t)
        return hit

    def rows_of_a(r):
        return av[lax.div(r, 2), :, pl.ds(pl.multiple_of(lax.rem(r, 2) * kb, 128), kb)]

    def step(s, this):
        for t, events in enumerate(steps):
            if events:
                @pl.when(s == t)
                def _():
                    for event in events:
                        handle(event)

        @pl.when(is_in(s, _FRESH))
        def _():
            fetch(s, this, True)

        after = decode(s + 1)

        @pl.when(jnp.logical_not(is_in(s, [t - 1 for t in _FRESH if t] + [len(steps) - 1])))
        def _():
            fetch(s + 1, after, True)

        fetch(s, this, False)
        r1, r2, n, h, final = this
        p = lax.rem(s, 2)
        for hh, (first, last) in enumerate(PIECES):
            @pl.when(h == hh)
            def _():
                for g in range(first, last):
                    col = n * PARTS + g
                    lhs = jnp.concatenate([rows_of_a(r1), rows_of_a(r2)], axis=1)
                    acc[col] += jnp.dot(
                        lhs, bbuf[p, :, pl.ds((g - first) * part, part)], preferred_element_type=jnp.float32)

                @pl.when(final == 1)
                def _():
                    for g in range(first, last):
                        col = n * PARTS + g
                        o_ref[:, pl.ds(pl.multiple_of(col * part, part), part)] = acc[col].astype(o_ref.dtype)
        return after

    lax.fori_loop(0, len(steps), step, decode(0))
    for n, (_, _, what, h) in enumerate(sent):
        ref = rows_piece(0, 0, h) if not isinstance(what, str) else av.at[0] if what in "LH" else transit.at[0]
        wait(ref, send_sem.at[n])


def solution(mesh):
    nx, ny, nc = mesh.shape["co"], mesh.shape["ri"], mesh.shape["ro"]

    def local_block(a, b):
        rows, (kb, nb) = a.shape[0] // nx, b.shape
        kd, part = a.shape[1], nb // PARTS
        dma = pltpu.SemaphoreType.DMA
        all_sends = set(first_sends())
        for event in sum(plan(), []):
            for near in range(2):
                all_sends.update(sends(event, near))
        out, _ = pl.pallas_call(
            functools.partial(kernel, nx, ny),
            out_shape=(
                pltpu.VMEM((rows, nx * nb), jnp.bfloat16),
                jax.ShapeDtypeStruct((nc * ny, nx, kb, nb), jnp.bfloat16),
            ),
            in_specs=[pl.BlockSpec(memory_space=pl.ANY)] * 2,
            out_specs=(pl.BlockSpec(memory_space=pltpu.VMEM), pl.BlockSpec(memory_space=pl.ANY)),
            scratch_shapes=[
                pltpu.VMEM((nx, rows, kd), jnp.bfloat16),
                pltpu.VMEM((2, rows // 2, kd), jnp.bfloat16),
                pltpu.VMEM((nx * PARTS, rows, part), jnp.float32),
                pltpu.VMEM((2, 2 * kb, FIRST * part), jnp.bfloat16),
                dma, dma((2,)), dma((2, 2)),
                dma((nc * ny, nx, 2)), dma, dma((6,)), dma((len(all_sends),)),
            ],
            compiler_params=pltpu.CompilerParams(
                collective_id=0, has_side_effects=True, vmem_limit_bytes=VMEM),
        )(a, b)
        return out

    return jax.shard_map(
        local_block,
        mesh=mesh,
        in_specs=(P(("dp", "ro", "ri"), "co"), P(("ro", "ri"), "co")),
        out_specs=P(("dp", "ro", "ri", "co"), None),
        check_vma=False,
    )
```

```python
import functools

import jax
import jax.numpy as jnp
from jax import lax
from jax.experimental import pallas as pl
from jax.experimental.pallas import tpu as pltpu
from jax.sharding import PartitionSpec as P

MESH = pl.DeviceIdType.MESH
VMEM = 48 * 1024 * 1024
PARTS = 5
FIRST = 3
PIECES = ((0, FIRST), (FIRST, PARTS))

_KINDS = (-1, 0, 1, 2, "side", "far")


def _unit(code):
    return _KINDS[code // 8], code // 2 % 4 - 1, code % 2


def _event(code):
    if isinstance(code, str):
        return code[0], len(code) - 1
    return (code // 8 - 1, code // 2 % 4 - 1), code % 2


_NEAR = [_unit(code) for code in (
    8, 16, 17, 9, 10, 25, 11, 12, 29, 27, 26, 24, 28, 30, 14, 13,
    31, 15, 39, 38, 0, 34, 4, 35, 20, 1, 5, 46, 21, 47, 42, 43,
)]
_FAR = [_unit(code) for code in (
    9, 16, 19, 8, 17, 0, 18, 3, 1, 21, 2, 4, 20, 5, 6, 22,
    23, 7, 25, 35, 34, 24, 12, 28, 38, 39, 13, 46, 29, 47, 42, 43,
)]

_EVENTS = [_event(code) for code in (
    2, 3, 18, 19, 5, "T", 4, 0, 1, "TT", 13, 6, 8, 9, 12, "L",
    7, 26, 21, 27, 20, "E", 16, "U", 17, "UU", 28, 24, 29, 25, "Z", 22,
    23, 30, 31, 14, 15,
)]
_COUNTS = [18, 1, 1, 0, 1, 2, 1, 1, 1, 1, 0, 0, 1, 0, 2, 0, 0, 1, 0, 1, 0, 0, 0, 0, 2, 0, 0, 2, 1, 0, 0, 0]
_FRESH = (0, 5)


def order(table):
    return table


def is_last(unit, near):
    k, i, _ = unit
    return k == "far" or (i == 1 and k in ((1, -1) if near else (0, 2)))


def plan():
    events = _EVENTS
    out = []
    for count in _COUNTS:
        out.append(events[:count])
        events = events[count:]
    assert not events
    return out


def sends(event, near):
    what, h = event
    out = []
    if what in ("T", "U"):
        out = [("x", 1, "F", h)]
        if h and not near:
            out += [("x", 1, "T", 0), ("x", 1, "T", 1), ("x", 1, "H", 0)]
        if h and near:
            out += [("x", 1, (-1, 2), q) for q in range(2)]
    if isinstance(what, str):
        return out
    if what == (-1, 0):
        if not near:
            out = [("x", 1, what, h)]
        out += [("y", 1, what, h), ("y", -1, what, h)]
        if h and near:
            out += [("x", 1, "T", 0), ("x", 1, "T", 1), ("x", 1, what, 0), ("x", 1, what, 1), ("x", 1, "H", 0)]
    if what == (-1, 2) and not near:
        out = [("x", 1, what, h)]
    if what == (1, 0) and h:
        out = [("y", -1, what, q) for q in range(2)]
    if what == (2, 0):
        out = [("y", -1, what, h)]
        if h:
            out += [("y", 1, what, q) for q in range(2)]
    if what == (-1, -1):
        out = [("y", 1, what, h)]
        if h:
            out += [("y", 1, (1, 0), q) for q in range(2)]
    if what == (1, -1):
        out = [("y", 1, what, h)]
        if h:
            out += [("y", 1, (0, -1), 0), ("y", 1, (0, -1), "q")]
    if what == (1, 2) and h:
        out = out + [("x", -1, (-1, 2), "t")]
    return out + [("c", 1, what, h)]


def first_sends():
    own = (0, 0)
    out = [(axis, s, own, h) for h in range(2) for s in (1, -1) for axis in "xy"]
    return out + [("x", -1, "L", 0)] + [("c", 1, own, h) for h in range(2)]


def kernel(nx, ny, a_ref, b_ref, o_ref, bg, av, transit, acc, bbuf,
           a_load, b_load, load_sem, recv_b, recv_q, recv_a, send_sem):
    x, y, c = lax.axis_index("co"), lax.axis_index("ri"), lax.axis_index("ro")
    d = 1 - 2 * c
    xs = lambda i: lax.rem(x + i * d + 2 * nx, nx)
    ys = lambda j: lax.rem(y + j * d + 2 * ny, ny)
    target = lambda axis, s: {"co": xs(s)} if axis == "x" else {"ri": ys(s)} if axis == "y" else {"ro": 1 - c}
    rows, (kb, nb) = av.shape[1], b_ref.shape
    part, half = nb // PARTS, rows // 2

    barrier = pltpu.get_barrier_semaphore()
    for who in (target("x", 1), target("x", -1), target("y", 1), target("y", -1), target("c", 1)):
        pl.semaphore_signal(barrier, inc=1, device_id=who, device_id_type=MESH)
    pl.semaphore_wait(barrier, 5)

    def cols(h):
        first, last = PIECES[h]
        return pl.ds(first * part, (last - first) * part)

    def row_of(j):
        return c * ny + ys(j)

    def piece(r, n, h):
        return bg.at[r, n, :, cols(h)]

    def a_rows(s, first, count):
        return a_ref.at[pl.ds(pl.multiple_of(xs(s) * rows + first, half), count)]

    def rows_piece(r, n, h):
        if h == "q":
            return bg.at[r, n, pl.ds(0, kb // 4), cols(1)]
        if h == "t":
            return bg.at[r, n, pl.ds(kb // 4, kb - kb // 4), cols(1)]
        return piece(r, n, h)

    sent = []

    def push(send):
        axis, s, what, h = send
        if send not in sent:
            sent.append(send)
        index = sent.index(send)
        if isinstance(what, str):
            at = pl.ds(h * half, half)
            if what == "L":
                src, dst, recv = a_rows(-1, 0, rows), av.at[x], 0
            elif what == "H":
                src, dst, recv = a_rows(1, 0, rows), av.at[x], 1
            elif what == "T":
                src, dst, recv = a_rows(2, h * half, half), transit.at[h], 2 + h
            else:
                src, dst, recv = transit.at[h], av.at[xs(-1), at], 4 + h
            sems = send_sem.at[index], recv_a.at[recv]
        else:
            i, j = what
            r, n = row_of(j), xs(i)
            dst = rows_piece(r, n, h)
            src = b_ref.at[:, cols(h)] if what == (0, 0) else dst
            sems = send_sem.at[index], recv_q if h == "q" else recv_b.at[r, n, 1 if h == "t" else h]
        pltpu.make_async_remote_copy(
            src_ref=src, dst_ref=dst, send_sem=sems[0], recv_sem=sems[1],
            device_id=target(axis, s), device_id_type=MESH).start()

    def wait(ref, sem):
        pltpu.make_async_copy(ref, ref, sem).wait()

    def wait_b(r, n, h):
        wait(piece(r, n, h), recv_b.at[r, n, h])

    near = lax.rem(x, 2) == lax.div(y, 2)

    def only(want, action):
        pl.when(near if want else jnp.logical_not(near))(action)

    def wait_behind():
        wait(av.at[xs(-1)], recv_a.at[1])

    def wait_across():
        for q in range(2):
            wait(av.at[xs(2), pl.ds(q * half, half)], recv_a.at[4 + q])

    def handle(event):
        what, h = event
        if what in ("T", "U"):
            @functools.partial(only, what == "U")
            def _():
                wait(transit.at[h], recv_a.at[2 + h])
                for send in sends(event, what == "U"):
                    push(send)
            return
        if what == "L":
            wait(av.at[xs(1)], recv_a.at[0])
        elif what in ("E", "Z"):
            only(what == "E", wait_across)
            only(what == "Z", wait_behind)
        else:
            i, j = what
            if what == (0, 2) and h:
                r, n = row_of(j), xs(i)
                wait(rows_piece(r, n, "q"), recv_q)
                wait(rows_piece(r, n, "t"), recv_b.at[r, n, h])
            else:
                wait_b(row_of(j), xs(i), h)
        both = [sends(event, want) for want in (False, True)]
        if both[0] == both[1]:
            for send in both[0]:
                push(send)
        else:
            for want in range(2):
                @functools.partial(only, want)
                def _():
                    for send in both[want]:
                        push(send)

    for send in first_sends():
        push(send)
    own_a = pltpu.make_async_copy(a_rows(0, 0, rows), av.at[x], a_load)
    own_a.start()
    own_b = [
        pltpu.make_async_copy(b_ref.at[:, cols(h)], bbuf.at[h, pl.ds(0, kb), pl.ds(0, cols(h).size)], b_load.at[h])
        for h in range(2)]
    for copy in own_b:
        copy.start()
    back = []
    for h in range(2):
        own_b[h].wait()
        back.append(pltpu.make_async_copy(
            bbuf.at[h, pl.ds(0, kb), pl.ds(0, cols(h).size)], piece(row_of(0), x, h), b_load.at[h]))
        back[h].start()

    def clear(n, _):
        acc[n] = jnp.zeros(acc.shape[1:], acc.dtype)
        return 0

    lax.fori_loop(0, acc.shape[0], clear, 0)
    for copy in back:
        copy.wait()
    own_a.wait()

    def unit(t):
        both = []
        for table, is_near in ((_FAR, False), (_NEAR, True)):
            k, i, h = order(table)[t]
            if isinstance(k, str):
                shift = ny // 2
                row = lax.rem(y + shift, ny)
                if k == "side":
                    row = lax.rem(y + 1 - 2 * lax.rem(y, 2) + shift, ny)
                fields = (row, row + ny, lax.rem(x + i, nx))
            else:
                k = xs(k)
                ro = lax.div(k, nx // 2)
                fields = (2 * k, 2 * k + 1, lax.rem(x + i * (1 - 2 * ro) + 2 * nx, nx))
            both.append(fields + (h, int(is_last(order(table)[t], is_near))))
        return [jnp.where(near, v, u) for u, v in zip(*both)]

    base, per = 1024, 3
    words = []
    for t in range(len(_COUNTS)):
        r1, r2, n, h, final = unit(t)
        code = (r1 + 8 * r2 + 64 * n + 256 * h + 512 * final) * base ** (t % per)
        if t % per:
            words[-1] += code
        else:
            words.append(code)

    def decode(s):
        w, m = lax.div(s, per), lax.rem(s, per)
        word = words[0]
        for n in range(1, len(words)):
            word = jnp.where(w == n, words[n], word)
        code = word
        for n in range(1, per):
            code = jnp.where(m == n, lax.div(word, base ** n), code)
        code = lax.rem(code, base)
        out = []
        for size in (8, 8, 4, 2, 2):
            out.append(lax.rem(code, size))
            code = lax.div(code, size)
        return tuple(out)

    def fetch(s, this, start):
        n, h = this[2], this[3]
        p = lax.rem(s, 2)
        for hh in range(2):
            @pl.when(h == hh)
            def _():
                for q in range(2):
                    r = this[q]
                    copy = pltpu.make_async_copy(
                        piece(r, n, hh), bbuf.at[p, pl.ds(q * kb, kb), pl.ds(0, cols(hh).size)], load_sem.at[p, q])
                    if start:
                        @pl.when(lax.div(r, ny) != c)
                        def _():
                            wait_b(r, n, hh)
                        copy.start()
                    else:
                        copy.wait()

    steps = plan()
    ahead = [t for t in range(1, len(steps)) if t not in _FRESH]

    def is_in(s, those):
        hit = s == those[0]
        for t in those[1:]:
            hit = jnp.logical_or(hit, s == t)
        return hit

    def rows_of_a(r):
        return av[lax.div(r, 2), :, pl.ds(pl.multiple_of(lax.rem(r, 2) * kb, 128), kb)]

    def step(s, this):
        for t, events in enumerate(steps):
            if events:
                @pl.when(s == t)
                def _():
                    for event in events:
                        handle(event)

        @pl.when(is_in(s, _FRESH))
        def _():
            fetch(s, this, True)

        after = decode(s + 1)

        @pl.when(jnp.logical_not(is_in(s, [t - 1 for t in _FRESH if t] + [len(steps) - 1])))
        def _():
            fetch(s + 1, after, True)

        fetch(s, this, False)
        r1, r2, n, h, final = this
        p = lax.rem(s, 2)
        for hh, (first, last) in enumerate(PIECES):
            def total(g, first=first):
                lhs = jnp.concatenate([rows_of_a(r1), rows_of_a(r2)], axis=1)
                rhs = bbuf[p, :, pl.ds((g - first) * part, part)]
                return acc[n * PARTS + g] + jnp.dot(lhs, rhs, preferred_element_type=jnp.float32)

            @pl.when(jnp.logical_and(h == hh, final == 0))
            def _():
                for g in range(first, last):
                    acc[n * PARTS + g] = total(g)

            @pl.when(jnp.logical_and(h == hh, final == 1))
            def _():
                for g in range(first, last):
                    at = pl.ds(pl.multiple_of((n * PARTS + g) * part, part), part)
                    o_ref[:, at] = total(g).astype(o_ref.dtype)
        return after

    lax.fori_loop(0, len(steps), step, decode(0))
    for n, (_, _, what, h) in enumerate(sent):
        ref = rows_piece(0, 0, h) if not isinstance(what, str) else av.at[0] if what in "LH" else transit.at[0]
        wait(ref, send_sem.at[n])


def solution(mesh):
    nx, ny, nc = mesh.shape["co"], mesh.shape["ri"], mesh.shape["ro"]

    def local_block(a, b):
        rows, (kb, nb) = a.shape[0] // nx, b.shape
        kd, part = a.shape[1], nb // PARTS
        dma = pltpu.SemaphoreType.DMA
        all_sends = set(first_sends())
        for event in sum(plan(), []):
            for near in range(2):
                all_sends.update(sends(event, near))
        out, _ = pl.pallas_call(
            functools.partial(kernel, nx, ny),
            out_shape=(
                pltpu.VMEM((rows, nx * nb), jnp.bfloat16),
                jax.ShapeDtypeStruct((nc * ny, nx, kb, nb), jnp.bfloat16),
            ),
            in_specs=[pl.BlockSpec(memory_space=pl.ANY)] * 2,
            out_specs=(pl.BlockSpec(memory_space=pltpu.VMEM), pl.BlockSpec(memory_space=pl.ANY)),
            scratch_shapes=[
                pltpu.VMEM((nx, rows, kd), jnp.bfloat16),
                pltpu.VMEM((2, rows // 2, kd), jnp.bfloat16),
                pltpu.VMEM((nx * PARTS, rows, part), jnp.float32),
                pltpu.VMEM((2, 2 * kb, FIRST * part), jnp.bfloat16),
                dma, dma((2,)), dma((2, 2)),
                dma((nc * ny, nx, 2)), dma, dma((6,)), dma((len(all_sends),)),
            ],
            compiler_params=pltpu.CompilerParams(
                collective_id=0, has_side_effects=True, vmem_limit_bytes=VMEM),
        )(a, b)
        return out

    return jax.shard_map(
        local_block,
        mesh=mesh,
        in_specs=(P(("dp", "ro", "ri"), "co"), P(("ro", "ri"), "co")),
        out_specs=P(("dp", "ro", "ri", "co"), None),
        check_vma=False,
    )
```
